32 devices in a mesh: groups: 2 (over y), seq: 4 (over z), mp: 2 (over x), sub: 2 (over core).
Axes of the slice: x: 2, y: 2, z: 4, core: 2. Of those that a mesh axis runs over, the one named last changes fastest.
Arguments:
- hidden_states: bfloat16 [2048, 8192], P(('groups', 'seq')), parts along dimension 0, may hold values from -8 to 8
- norm_gain: float32 [8192], replicated, may hold values from 0.25 to 1.75
- w_query: bfloat16 [8192, 2048], P('seq', ('mp', 'sub')), may hold values from -14 to 14
- w_keyval: bfloat16 [8192, 512], P('seq', ('mp', 'sub')), may hold values from -1 to 1
- doc_lengths: int32 [16], P('groups'), parts along dimension 0, may hold values from 1 to 512, 1024 in all
Outputs:
- attended: bfloat16 [2048, 2048], P(('groups', 'seq'), ('mp', 'sub')), parts along dimension 0
The draws below stay inside these ranges and needn't reach their ends.
There are 2 independent parts, one for each index of `groups`. The reference program is written for one: setup_inputs(seed, part) draws one part's arguments, and reference() takes and returns one part's arrays. A program takes and returns all parts, laid end to end along the dimension named above; an argument that names none is the same for every part. Nothing has to cross between parts.
Inputs may be any that keep to these rules, and one draw needn't show every extreme that they name: `doc_lengths`: the lengths sum to 1024 and the longest is exactly 512.
All inputs are finite; a program needn't handle non-finite values.
Results may differ from the reference program's by a relative error of at most 0.0079.
Values may be sent and summed in bfloat16 or wider, within the bound.
No kernel may reach another device: no remote copies, remote signals or barrier semaphores. Data moves between devices by JAX's collectives and lax.ppermute only.
A program may use at most 64 MiB of HBM per device.

```python
import math
import jax
import jax.numpy as jnp
import numpy as np
from jax import lax

D = 8192
HEAD_DIM = 128
GROUP = 8
DOCS = 8
KV_HEADS = 2
Q_HEADS = 16
TOKENS = 1024


def projection_pair(key):
    factor = 1.0 / math.sqrt(D)
    keyval = jnp.clip(jax.random.normal(jax.random.fold_in(key, 11), (D, KV_HEADS, 2, HEAD_DIM), jnp.float32), -4.0, 4.0) * factor
    query_part = jnp.clip(jax.random.normal(jax.random.fold_in(key, 12), (D, Q_HEADS, HEAD_DIM), jnp.float32), -4.0, 4.0) * factor
    return (query_part.reshape(D, Q_HEADS * HEAD_DIM), keyval.reshape(D, 2 * KV_HEADS * HEAD_DIM))


def draw_w_query(key, part):
    return projection_pair(key)[0].astype(jnp.bfloat16)


def draw_w_keyval(key, part):
    return projection_pair(key)[1].astype(jnp.bfloat16)


def draw_hidden_states(key, part):
    drawn = jax.random.normal(jax.random.fold_in(key, 24), (TOKENS, D), jnp.float32)
    return jnp.clip(drawn, -6.0, 6.0).astype(jnp.bfloat16)


def profile(count, total, bound, slope):
    loads = [(1 << 20) // math.isqrt(rank ** slope) + 1 for rank in range(2, count + 1)]
    surplus, holding = total - bound - (count - 1), [1] * (count - 1)
    while surplus > 0:
        candidates = [i for i in range(count - 1) if holding[i] < bound]
        mass, left = sum([loads[i] for i in candidates]), surplus
        for i in candidates:
            addition = min(bound - holding[i], max(1, left * loads[i] // mass), surplus)
            holding[i] = holding[i] + addition
            surplus = surplus - addition
    return np.array([bound] + holding)


def uneven(own_key, number_of, total, reach, lean):
    if number_of == 2:
        one = jax.random.randint(own_key, (), max(1, total - reach), min(reach, total - 1) + 1)
        return jnp.stack([one, total - one])
    sizes = jnp.asarray(profile(number_of, total, reach, lean), jnp.int32)
    pairs = (number_of - 1) // 2
    source_of, receiver = sizes[1:1 + 2 * pairs:2], sizes[2:2 + 2 * pairs:2]
    slack = jnp.minimum(source_of - 1, reach - receiver)
    moved = jax.random.randint(jax.random.fold_in(own_key, 1), (pairs,), 0, 1 << 20) % (slack + 1)
    sizes = sizes.at[1:1 + 2 * pairs:2].set(source_of - moved).at[2:2 + 2 * pairs:2].set(receiver + moved)
    return sizes[jax.random.permutation(jax.random.fold_in(own_key, 2), number_of)]


def setup_inputs(seed: int = 0, part: int = 0) -> dict:
    key_list = jax.random.split(jax.random.key(seed), 6)
    own_keys = jax.random.split(jax.random.fold_in(key_list[5], part), 6)
    return {
        "hidden_states": draw_hidden_states(jax.random.fold_in(jax.random.fold_in(key_list[5], part), 71), part),
        "norm_gain": jnp.clip(1.0 + 0.15 * jax.random.normal(key_list[1], (D,), jnp.float32), 0.25, 1.75),
        "w_query": draw_w_query(jax.random.fold_in(key_list[5], 71), part),
        "w_keyval": draw_w_keyval(jax.random.fold_in(key_list[5], 71), part),
        "doc_lengths": uneven(own_keys[4], DOCS, TOKENS, TOKENS // 2, 2).astype(jnp.int32),
    }


NEG_LARGE = -1e+30
ROPE_BASE = 500000.0

def rms_norm(states, gain):
    as_float = states.astype(jnp.float32)
    factor = lax.rsqrt(lax.optimization_barrier(jnp.mean(as_float * as_float, axis=-1, keepdims=True)) + 1e-05)
    return (as_float * factor * gain[None, :].astype(jnp.float32)).astype(jnp.bfloat16)

def token_starts(positions, doc_lengths):
    doc_ends = jnp.cumsum(doc_lengths)
    begins = doc_ends - doc_lengths
    inside = begins[None, :] <= positions[:, None]
    return lax.optimization_barrier(jnp.max(jnp.where(inside, begins[None, :], 0), axis=1)).astype(jnp.int32)

def rope_tables(inner):
    half_dim = HEAD_DIM // 2
    frequency = jnp.exp(jnp.arange(half_dim, dtype=jnp.float32) * (-2.0 * math.log(ROPE_BASE) / HEAD_DIM))
    angle = inner.astype(jnp.float32)[:, None] * frequency[None, :]
    return (jnp.cos(angle)[:, None, :], jnp.sin(angle)[:, None, :])

def rotate(vectors, cosine, sine_table):
    half_dim = vectors.shape[-1] // 2
    first_half = vectors[..., :half_dim]
    second_half = vectors[..., half_dim:]
    return jnp.concatenate([first_half * cosine - second_half * sine_table, second_half * cosine + first_half * sine_table], axis=-1)

def reference(hidden_states, norm_gain, w_query, w_keyval, doc_lengths):
    positions = jnp.arange(TOKENS, dtype=jnp.int32)
    starts = token_starts(positions, doc_lengths)
    cosine, sine_table = rope_tables(positions - starts)
    normed = rms_norm(hidden_states, norm_gain)
    query_sum = jnp.dot(normed, w_query, preferred_element_type=jnp.float32)
    keyval_sum = jnp.dot(normed, w_keyval, preferred_element_type=jnp.float32)
    queries = rotate(query_sum.reshape(TOKENS, Q_HEADS, HEAD_DIM), cosine, sine_table).astype(jnp.bfloat16)
    paired = keyval_sum.reshape(TOKENS, KV_HEADS, 2, HEAD_DIM)
    keys = rotate(paired[:, :, 0, :], cosine, sine_table).astype(jnp.bfloat16)
    values = paired[:, :, 1, :].astype(jnp.bfloat16)
    allowed = (positions[None, :] >= starts[:, None]) & (positions[None, :] <= positions[:, None])
    softmax_scale = 1.0 / math.sqrt(HEAD_DIM)

    def one_head(head_index):
        kv_index = head_index // GROUP
        head_query = lax.dynamic_index_in_dim(queries, head_index, 1, keepdims=False)
        head_keys = lax.dynamic_index_in_dim(keys, kv_index, 1, keepdims=False)
        head_values = lax.dynamic_index_in_dim(values, kv_index, 1, keepdims=False)
        scores = jnp.dot(head_query, head_keys.T, preferred_element_type=jnp.float32) * softmax_scale
        scores = jnp.where(allowed, scores, NEG_LARGE)
        row_max = lax.optimization_barrier(jnp.max(scores, axis=-1, keepdims=True))
        exponent = jnp.where(allowed, jnp.exp(scores - row_max), 0.0)
        summed = jnp.dot(exponent.astype(jnp.bfloat16), head_values, preferred_element_type=jnp.float32)
        return (summed / lax.optimization_barrier(jnp.sum(exponent, axis=-1, keepdims=True))).astype(jnp.bfloat16)
    heads = lax.map(one_head, jnp.arange(Q_HEADS, dtype=jnp.int32))
    return jnp.transpose(heads, (1, 0, 2)).reshape(TOKENS, Q_HEADS * HEAD_DIM)
```

```python
import math

import jax
import jax.numpy as jnp
from jax import lax
from jax.sharding import PartitionSpec as P

HEAD_DIM = 128


NEG_LARGE = -1e30
ROPE_BASE = 500000.0
W_BOUND = 14.0
GAIN_BOUND = 1.75
WIRE_MAX = 60000.0


def rms_norm(states, gain):
    as_float = states.astype(jnp.float32)
    factor = lax.rsqrt(jnp.mean(as_float * as_float, axis=-1, keepdims=True) + 1e-05)
    return (as_float * factor * gain[None, :]).astype(jnp.bfloat16)


def token_starts(positions, doc_lengths):
    doc_ends = jnp.cumsum(doc_lengths)
    begins = doc_ends - doc_lengths
    inside = begins[None, :] <= positions[:, None]
    return jnp.max(jnp.where(inside, begins[None, :], 0), axis=1)


def rope_tables(inner):
    half_dim = HEAD_DIM // 2
    frequency = jnp.exp(
        jnp.arange(half_dim, dtype=jnp.float32) * (-2.0 * math.log(ROPE_BASE) / HEAD_DIM)
    )
    angle = inner.astype(jnp.float32)[:, None] * frequency[None, :]
    return (jnp.cos(angle)[:, None, :], jnp.sin(angle)[:, None, :])


def rotate(vectors, cosine, sine_table):
    half_dim = vectors.shape[-1] // 2
    first_half = vectors[..., :half_dim]
    second_half = vectors[..., half_dim:]
    return jnp.concatenate(
        [
            first_half * cosine - second_half * sine_table,
            second_half * cosine + first_half * sine_table,
        ],
        axis=-1,
    )


def pull(array, axis, shift, size):
    pairs = [((i + shift) % size, i) for i in range(size)]
    return lax.ppermute(array, axis, pairs)


def dot(a, b):
    return jnp.dot(a, b, preferred_element_type=jnp.float32)


def shards(sizes, hidden_states, norm_gain, w_query, w_keyval, doc_lengths):
    n, m_size, c_size = sizes["seq"], sizes["mp"], sizes["sub"]
    quarters = m_size * c_size
    row_count, width = hidden_states.shape
    depth = w_query.shape[0]
    piece = depth // quarters
    s, m, c = lax.axis_index("seq"), lax.axis_index("mp"), lax.axis_index("sub")
    positions = s * row_count + jnp.arange(row_count, dtype=jnp.int32)
    starts = token_starts(positions, doc_lengths)
    cosine, sine_table = rope_tables(positions - starts)
    normed = rms_norm(hidden_states, norm_gain)

    bound = GAIN_BOUND * math.sqrt(width) * W_BOUND * math.sqrt(depth)
    wire_scale = 2.0 ** min(0, math.floor(math.log2(WIRE_MAX / bound)))

    offsets = sorted(range(1, n), key=lambda d: min(d, n - d))
    quarter = m * c_size + c
    arrived = {}
    for d in offsets:
        to = lax.rem(s + d, n)
        mine = lax.dynamic_slice_in_dim(normed, to * depth + quarter * piece, piece, 1)
        arrived[d] = pull(mine, "seq", -d, n)
    order = [(i, j) for i in range(m_size) for j in range(c_size)]
    row_starts = [
        (lax.rem(m + i, m_size) * c_size + lax.rem(c + j, c_size)) * piece for i, j in order
    ]
    wq_turned = jnp.concatenate(
        [lax.dynamic_slice_in_dim(w_query, r, piece, 0) for r in row_starts], axis=0
    )
    wkv_turned = jnp.concatenate(
        [lax.dynamic_slice_in_dim(w_keyval, r, piece, 0) for r in row_starts], axis=0
    )
    own = lax.dynamic_slice_in_dim(normed, s * depth, depth, 1)
    keyval_sum = dot(own, w_keyval)
    query_sum = dot(own, w_query)
    q_parts, kv_parts = [], []
    for d in offsets:
        parts = {(0, 0): arrived[d]}
        for i in range(1, m_size):
            parts[i, 0] = pull(arrived[d], "mp", i, m_size)
        for i in range(m_size):
            for j in range(1, c_size):
                parts[i, j] = pull(parts[i, 0], "sub", j, c_size)
        block = jnp.concatenate([parts[o] for o in order], axis=1)
        kv_part = (dot(block, wkv_turned) * wire_scale).astype(jnp.float16)
        q_part = (dot(block, wq_turned) * wire_scale).astype(jnp.float16)
        kv_parts.append(pull(kv_part, "seq", d, n))
        q_parts.append(pull(q_part, "seq", d, n))
    unscale = 1.0 / wire_scale
    for part in kv_parts:
        keyval_sum = keyval_sum + part.astype(jnp.float32) * unscale
    for part in q_parts:
        query_sum = query_sum + part.astype(jnp.float32) * unscale

    is_key = c == 0
    rotated = rotate(keyval_sum[:, None, :], cosine, sine_table)[:, 0, :]
    own_half = jnp.where(is_key, rotated, keyval_sum).astype(jnp.bfloat16)
    reach = n // 2
    halves = [
        lax.ppermute(own_half, "seq", [(i, i + e) for i in range(n - e)])
        for e in range(reach, 0, -1)
    ] + [own_half]
    half = jnp.concatenate(halves, axis=0)
    other = lax.ppermute(half, "sub", [(j, 1 - j) for j in range(c_size)])
    all_keys = jnp.where(is_key, half, other)
    values = jnp.where(is_key, other, half)

    queries = rotate(query_sum.reshape(row_count, -1, HEAD_DIM), cosine, sine_table).astype(
        jnp.bfloat16
    )
    head_count = queries.shape[1]
    key_position = (s - reach) * row_count + jnp.arange(all_keys.shape[0], dtype=jnp.int32)
    allowed = (
        (key_position[None, :] >= starts[:, None]) & (key_position[None, :] <= positions[:, None])
    )[None, :, :]
    softmax_scale = 1.0 / math.sqrt(HEAD_DIM)
    scores = (
        jnp.einsum("thd,kd->htk", queries, all_keys, preferred_element_type=jnp.float32)
        * softmax_scale
    )
    scores = jnp.where(allowed, scores, NEG_LARGE)
    top = jnp.max(scores, axis=-1, keepdims=True)
    weights = jnp.where(allowed, jnp.exp(scores - top), 0.0)
    total = jnp.sum(weights, axis=-1)
    summed = jnp.einsum(
        "htk,kd->htd", weights.astype(jnp.bfloat16), values, preferred_element_type=jnp.float32
    )
    attended = (summed / total[..., None]).transpose(1, 0, 2)
    return attended.reshape(row_count, head_count * HEAD_DIM).astype(jnp.bfloat16)


def solution(mesh):
    in_specs = (
        P(("groups", "seq"), None),
        P(),
        P("seq", ("mp", "sub")),
        P("seq", ("mp", "sub")),
        P("groups"),
    )
    out_specs = P(("groups", "seq"), ("mp", "sub"))
    sizes = dict(mesh.shape)

    def body(*arrays):
        return shards(sizes, *arrays)

    return jax.shard_map(body, mesh=mesh, in_specs=in_specs, out_specs=out_specs, check_vma=False)
```

```python
import functools
import math

import jax
import jax.numpy as jnp
from jax import lax
from jax.experimental import pallas as pl
from jax.experimental.pallas import tpu as pltpu
from jax.sharding import PartitionSpec as P

HEAD_DIM = 128


NEG_LARGE = -1e30
ROPE_BASE = 500000.0
W_BOUND = 14.0
GAIN_BOUND = 1.75
WIRE_MAX = 60000.0


def norm_kernel(columns, hidden_ref, gain_ref, *out_refs):
    as_float = hidden_ref[...].astype(jnp.float32)
    factor = lax.rsqrt(jnp.mean(as_float * as_float, axis=-1, keepdims=True) + 1e-05)
    for k, out_ref in enumerate(out_refs):
        chosen = pl.ds(pl.multiple_of(columns[k], 128), out_ref.shape[1])
        part = hidden_ref[:, chosen].astype(jnp.float32)
        out_ref[...] = (part * factor * gain_ref[:, chosen]).astype(jnp.bfloat16)


def normed_columns(states, gain, starts, widths):
    rows, width = states.shape
    if any(w % 128 for w in widths):
        as_float = states.astype(jnp.float32)
        factor = lax.rsqrt(jnp.mean(as_float * as_float, axis=-1, keepdims=True) + 1e-05)
        normed = (as_float * factor * gain[None, :]).astype(jnp.bfloat16)
        return [lax.dynamic_slice_in_dim(normed, s, w, 1) for s, w in zip(starts, widths)]
    tile = min(32, rows)
    return pl.pallas_call(
        norm_kernel,
        out_shape=[jax.ShapeDtypeStruct((rows, w), jnp.bfloat16) for w in widths],
        grid_spec=pltpu.PrefetchScalarGridSpec(
            num_scalar_prefetch=1,
            grid=(rows // tile,),
            in_specs=[
                pl.BlockSpec((tile, width), lambda i, _: (i, 0)),
                pl.BlockSpec((1, width), lambda i, _: (0, 0)),
            ],
            out_specs=[pl.BlockSpec((tile, w), lambda i, _: (i, 0)) for w in widths],
        ),
        cost_estimate=pl.CostEstimate(
            flops=6 * rows * width, bytes_accessed=3 * rows * width, transcendentals=rows
        ),
        name="norm",
    )(jnp.stack(starts).astype(jnp.int32), states, gain[None, :])


def attend_kernel(reach, scalars, start_ref, query_ref, half_ref, other_ref, out_ref):
    rows, count = query_ref.shape[0], half_ref.shape[0]
    is_key = scalars[1] == 0
    keys = jnp.where(is_key, half_ref[...], other_ref[...])
    values = jnp.where(is_key, other_ref[...], half_ref[...])
    first = scalars[0] * rows
    shape = (rows, count)
    position = first + lax.broadcasted_iota(jnp.int32, shape, 0)
    key_position = first - reach * rows + lax.broadcasted_iota(jnp.int32, shape, 1)
    allowed = (key_position >= start_ref[...]) & (key_position <= position)
    scores = lax.dot_general(
        query_ref[...], keys, (((1,), (1,)), ((), ())), preferred_element_type=jnp.float32
    ) * (1.0 / math.sqrt(HEAD_DIM))
    scores = jnp.where(allowed, scores, NEG_LARGE)
    top = jnp.max(scores, axis=-1, keepdims=True)
    weights = jnp.where(allowed, jnp.exp(scores - top), 0.0)
    total = jnp.sum(weights, axis=-1, keepdims=True)
    summed = jnp.dot(weights.astype(jnp.bfloat16), values, preferred_element_type=jnp.float32)
    out_ref[...] = (summed / total).astype(jnp.bfloat16)


def attend(reach, scalars, starts, queries, half, other):
    rows, columns = queries.shape
    count = half.shape[0]
    heads = columns // HEAD_DIM
    whole = pl.BlockSpec((count, HEAD_DIM), lambda h, _: (0, 0))
    per_head = pl.BlockSpec((rows, HEAD_DIM), lambda h, _: (0, h))
    return pl.pallas_call(
        functools.partial(attend_kernel, reach),
        out_shape=jax.ShapeDtypeStruct(queries.shape, jnp.bfloat16),
        grid_spec=pltpu.PrefetchScalarGridSpec(
            num_scalar_prefetch=1,
            grid=(heads,),
            in_specs=[pl.BlockSpec((rows, 1), lambda h, _: (0, 0)), per_head, whole, whole],
            out_specs=per_head,
        ),
        cost_estimate=pl.CostEstimate(
            flops=4 * rows * count * columns,
            bytes_accessed=4 * rows * columns + 4 * count * HEAD_DIM,
            transcendentals=rows * count * heads,
        ),
        name="attend",
    )(scalars, starts[:, None], queries, half, other)


def token_starts(positions, doc_lengths):
    doc_ends = jnp.cumsum(doc_lengths)
    begins = doc_ends - doc_lengths
    inside = begins[None, :] <= positions[:, None]
    return jnp.max(jnp.where(inside, begins[None, :], 0), axis=1)


def rope_tables(inner):
    half_dim = HEAD_DIM // 2
    frequency = jnp.exp(
        jnp.arange(half_dim, dtype=jnp.float32) * (-2.0 * math.log(ROPE_BASE) / HEAD_DIM)
    )
    angle = inner.astype(jnp.float32)[:, None] * frequency[None, :]
    return (jnp.cos(angle)[:, None, :], jnp.sin(angle)[:, None, :])


def rotate(vectors, cosine, sine_table):
    half_dim = vectors.shape[-1] // 2
    first_half = vectors[..., :half_dim]
    second_half = vectors[..., half_dim:]
    return jnp.concatenate(
        [
            first_half * cosine - second_half * sine_table,
            second_half * cosine + first_half * sine_table,
        ],
        axis=-1,
    )


def pull(array, axis, shift, size):
    pairs = [((i + shift) % size, i) for i in range(size)]
    return lax.ppermute(array, axis, pairs)


def dot(a, b):
    return jnp.dot(a, b, preferred_element_type=jnp.float32)


def offsets_of(n):
    return sorted(range(1, n), key=lambda d: min(d, n - d))


def shards(sizes, hidden_states, norm_gain, w_query, w_keyval, doc_lengths):
    n, m_size, c_size = sizes["seq"], sizes["mp"], sizes["sub"]
    quarters = m_size * c_size
    row_count, width = hidden_states.shape
    depth = w_query.shape[0]
    piece = depth // quarters
    s, m, c = lax.axis_index("seq"), lax.axis_index("mp"), lax.axis_index("sub")
    offsets = offsets_of(n)

    bound = GAIN_BOUND * math.sqrt(width) * W_BOUND * math.sqrt(depth)
    wire_scale = 2.0 ** min(0, math.floor(math.log2(WIRE_MAX / bound)))

    quarter = m * c_size + c
    columns = [lax.rem(s + d, n) * depth + quarter * piece for d in offsets] + [s * depth]
    widths = [piece] * len(offsets) + [depth]
    *mine, own = normed_columns(hidden_states, norm_gain, columns, widths)
    arrived = {d: pull(part, "seq", -d, n) for d, part in zip(offsets, mine)}

    positions = s * row_count + jnp.arange(row_count, dtype=jnp.int32)
    starts = token_starts(positions, doc_lengths)
    cosine, sine_table = rope_tables(positions - starts)

    turned = []
    for j in range(c_size):
        for i in range(m_size):
            place = lax.rem(m + i, m_size) * c_size + lax.rem(c + j, c_size)
            rows = place * piece
            turned.append((lax.dynamic_slice_in_dim(w_query, rows, piece, 0),
                           lax.dynamic_slice_in_dim(w_keyval, rows, piece, 0)))
    wq_turned = jnp.concatenate([q for q, _ in turned], axis=0)
    wkv_turned = jnp.concatenate([kv for _, kv in turned], axis=0)
    keyval_sum = dot(own, w_keyval)
    query_sum = dot(own, w_query)
    q_parts, kv_parts = [], []
    for d in offsets:
        near = [arrived[d]] + [pull(arrived[d], "mp", i, m_size) for i in range(1, m_size)]
        near = jnp.concatenate(near, axis=1)
        block = [near] + [pull(near, "sub", j, c_size) for j in range(1, c_size)]
        step = near.shape[1]
        kv_part = sum(dot(b, wkv_turned[j * step : (j + 1) * step]) for j, b in enumerate(block))
        q_part = sum(dot(b, wq_turned[j * step : (j + 1) * step]) for j, b in enumerate(block))
        kv_part = (kv_part * wire_scale).astype(jnp.float16)
        q_part = (q_part * wire_scale).astype(jnp.float16)
        kv_parts.append(pull(kv_part, "seq", d, n))
        q_parts.append(pull(q_part, "seq", d, n))
    unscale = 1.0 / wire_scale
    for part in kv_parts:
        keyval_sum = keyval_sum + part.astype(jnp.float32) * unscale
    for part in q_parts:
        query_sum = query_sum + part.astype(jnp.float32) * unscale

    rotated = rotate(keyval_sum[:, None, :], cosine, sine_table)[:, 0, :]
    own_half = jnp.where(c == 0, rotated, keyval_sum).astype(jnp.bfloat16)
    reach = n // 2
    halves = []
    for e in range(reach, 0, -1):
        halves.append(lax.ppermute(own_half, "seq", [(i, i + e) for i in range(n - e)]))
    half = jnp.concatenate(halves + [own_half], axis=0)
    other = pull(half, "sub", 1, c_size)
    queries = rotate(query_sum.reshape(row_count, -1, HEAD_DIM), cosine, sine_table)
    queries = queries.astype(jnp.bfloat16).reshape(row_count, -1)
    return attend(reach, jnp.stack([s, c]), starts, queries, half, other)


def solution(mesh):
    in_specs = (
        P(("groups", "seq"), None),
        P(),
        P("seq", ("mp", "sub")),
        P("seq", ("mp", "sub")),
        P("groups"),
    )
    out_specs = P(("groups", "seq"), ("mp", "sub"))
    sizes = dict(mesh.shape)

    def body(*arrays):
        return shards(sizes, *arrays)

    return jax.shard_map(body, mesh=mesh, in_specs=in_specs, out_specs=out_specs, check_vma=False)
```

```python
import functools
import math

import jax
import jax.numpy as jnp
from jax import lax
from jax.experimental import pallas as pl
from jax.experimental.pallas import tpu as pltpu
from jax.sharding import PartitionSpec as P

HEAD_DIM = 128


NEG_LARGE = -1e30
ROPE_BASE = 500000.0
W_BOUND = 14.0
GAIN_BOUND = 1.75
WIRE_MAX = 60000.0


def inverse_norm(states):
    as_float = states.astype(jnp.float32)
    return lax.rsqrt(jnp.mean(as_float * as_float, axis=-1) + 1e-05)


def scaled(states, factor, gain):
    return (states.astype(jnp.float32) * factor[:, None] * gain[None, :]).astype(jnp.bfloat16)


def token_starts(positions, doc_lengths):
    doc_ends = jnp.cumsum(doc_lengths)
    begins = doc_ends - doc_lengths
    inside = begins[None, :] <= positions[:, None]
    return jnp.max(jnp.where(inside, begins[None, :], 0), axis=1)


def rope_tables(inner):
    half_dim = HEAD_DIM // 2
    frequency = jnp.exp(
        jnp.arange(half_dim, dtype=jnp.float32) * (-2.0 * math.log(ROPE_BASE) / HEAD_DIM)
    )
    angle = inner.astype(jnp.float32)[:, None] * frequency[None, :]
    cosine, sine = jnp.cos(angle), jnp.sin(angle)
    return (
        jnp.concatenate([cosine, cosine], axis=1),
        jnp.concatenate([-sine, sine], axis=1),
    )


def attend_kernel(
    reach, chunk, docs, scalars, query_ref, cos_ref, sin_ref, half_ref, other_ref, out_ref
):
    rows, count = query_ref.shape[0], half_ref.shape[0]
    heads = query_ref.shape[1] // HEAD_DIM
    first, is_key = scalars[0] * rows, scalars[1] == 0
    exponent_scale = math.log2(math.e) / math.sqrt(HEAD_DIM)
    column = first + lax.broadcasted_iota(jnp.int32, (rows, 1), 0)
    start = jnp.zeros((rows, 1), jnp.int32)
    begin = 0
    for k in range(docs):
        start = jnp.where(column >= begin, begin, start)
        begin = begin + scalars[2 + k]
    queries = []
    for h in range(heads):
        u = query_ref[:, h * HEAD_DIM : (h + 1) * HEAD_DIM]
        turned = pltpu.roll(u, HEAD_DIM // 2, 1)
        queries.append((u * cos_ref[...] + turned * sin_ref[...]).astype(jnp.bfloat16))
    for a in range(0, rows, chunk):
        low = (a + 1) // 128 * 128
        high = min(count, -(-(reach * rows + a + chunk) // 128) * 128)
        shape = (chunk, high - low)
        position = first + a + lax.broadcasted_iota(jnp.int32, shape, 0)
        key_position = first - reach * rows + low + lax.broadcasted_iota(jnp.int32, shape, 1)
        allowed = (key_position >= start[a : a + chunk]) & (key_position <= position)
        allowed = jnp.concatenate([allowed] * heads, axis=0)
        keys = jnp.where(is_key, half_ref[low:high, :], other_ref[low:high, :])
        values = jnp.where(is_key, other_ref[low:high, :], half_ref[low:high, :])
        query = jnp.concatenate([q[a : a + chunk] for q in queries], axis=0)
        scores = lax.dot_general(
            query, keys, (((1,), (1,)), ((), ())), preferred_element_type=jnp.float32
        )
        scores = jnp.where(allowed, scores, NEG_LARGE)
        top = jnp.max(scores, axis=-1, keepdims=True)
        weights = jnp.where(allowed, jnp.exp2((scores - top) * exponent_scale), 0.0)
        total = jnp.sum(weights, axis=-1, keepdims=True)
        summed = jnp.dot(weights.astype(jnp.bfloat16), values, preferred_element_type=jnp.float32)
        result = (summed / total).astype(jnp.bfloat16)
        for h in range(heads):
            columns = slice(h * HEAD_DIM, (h + 1) * HEAD_DIM)
            out_ref[a : a + chunk, columns] = result[h * chunk : (h + 1) * chunk]


def attend(reach, docs, scalars, query_sum, cosine, sine, half, other):
    rows, columns = query_sum.shape
    count = half.shape[0]
    chunk = rows
    while chunk > 16 and chunk * columns // HEAD_DIM * count > (1 << 19):
        chunk //= 2
    return pl.pallas_call(
        functools.partial(attend_kernel, reach, chunk, docs),
        out_shape=jax.ShapeDtypeStruct(query_sum.shape, jnp.bfloat16),
        in_specs=[pl.BlockSpec(memory_space=pltpu.SMEM)]
        + [pl.BlockSpec(memory_space=pltpu.VMEM)] * 5,
        out_specs=pl.BlockSpec(memory_space=pltpu.VMEM),
        cost_estimate=pl.CostEstimate(
            flops=4 * rows * count * columns,
            bytes_accessed=8 * rows * columns + 4 * count * HEAD_DIM,
            transcendentals=rows * count * columns // HEAD_DIM,
        ),
        name="attend",
    )(scalars, query_sum, cosine, sine, half, other)


def pull(array, axis, shift, size):
    pairs = [((i + shift) % size, i) for i in range(size)]
    return lax.ppermute(array, axis, pairs)


def dot(a, b):
    return jnp.dot(a, b, preferred_element_type=jnp.float32)


def stages_of(n):
    return [sorted({d, n - d}) for d in range(1, n // 2 + 1)]


def shards(sizes, hidden_states, norm_gain, w_query, w_keyval, doc_lengths):
    n, m_size, c_size = sizes["seq"], sizes["mp"], sizes["sub"]
    quarters = m_size * c_size
    row_count, width = hidden_states.shape
    depth = w_query.shape[0]
    piece = depth // quarters
    s, m, c = lax.axis_index("seq"), lax.axis_index("mp"), lax.axis_index("sub")
    stages = stages_of(n)

    bound = GAIN_BOUND * math.sqrt(width) * W_BOUND * math.sqrt(depth)
    wire_scale = 2.0 ** min(0, math.floor(math.log2(WIRE_MAX / bound)))
    unscale = 1.0 / wire_scale

    quarter = m * c_size + c
    arrived = {}
    for stage in stages:
        for d in stage:
            column = lax.rem(s + d, n) * depth + quarter * piece
            mine = lax.dynamic_slice_in_dim(hidden_states, column, piece, 1)
            arrived[d] = pull(mine, "seq", -d, n)
    factor = inverse_norm(hidden_states)
    factors = {d: pull(factor, "seq", -d, n) for stage in stages for d in stage}
    own = scaled(
        lax.dynamic_slice_in_dim(hidden_states, s * depth, depth, 1),
        factor,
        lax.dynamic_slice_in_dim(norm_gain, s * depth, depth, 0),
    )
    gain_piece = lax.dynamic_slice_in_dim(norm_gain, s * depth + quarter * piece, piece, 0)

    positions = s * row_count + jnp.arange(row_count, dtype=jnp.int32)
    starts = token_starts(positions, doc_lengths)
    cosine, sine = rope_tables(positions - starts)
    scalars = jnp.concatenate([jnp.stack([s, c]).astype(jnp.int32), doc_lengths])

    turned = []
    for j in range(c_size):
        for i in range(m_size):
            place = lax.rem(m + i, m_size) * c_size + lax.rem(c + j, c_size)
            rows = place * piece
            turned.append((lax.dynamic_slice_in_dim(w_query, rows, piece, 0),
                           lax.dynamic_slice_in_dim(w_keyval, rows, piece, 0)))
    step = m_size * piece
    wq_turned = jnp.concatenate([q for q, _ in turned], axis=0)
    wkv_turned = jnp.concatenate([kv for _, kv in turned], axis=0)
    keyval_sum = dot(own, w_keyval)
    query_sum = dot(own, w_query)
    q_parts, kv_parts = [], []
    for k, stage in enumerate(stages):
        for d in stage if k else []:
            arrived[d], _ = lax.optimization_barrier((arrived[d], first))
        first = jnp.concatenate([scaled(arrived[d], factors[d], gain_piece) for d in stage], axis=0)
        near = [first] + [pull(first, "mp", i, m_size) for i in range(1, m_size)]
        near = jnp.concatenate(near, axis=1)
        block = [near] + [pull(near, "sub", j, c_size) for j in range(1, c_size)]
        kvs, qs = [], []
        for i in range(len(stage)):
            parts = [b[i * row_count : (i + 1) * row_count] for b in block]
            rows = [slice(j * step, (j + 1) * step) for j in range(c_size)]
            kv_part = sum(dot(part, wkv_turned[r]) for part, r in zip(parts, rows))
            q_part = sum(dot(part, wq_turned[r]) for part, r in zip(parts, rows))
            kvs.append((kv_part * wire_scale).astype(jnp.float16))
            qs.append((q_part * wire_scale).astype(jnp.float16))
        kv_parts += [pull(part, "seq", d, n) for d, part in zip(stage, kvs)]
        q_parts += [pull(part, "seq", d, n) for d, part in zip(stage, qs)]
    for part in kv_parts:
        keyval_sum = keyval_sum + part.astype(jnp.float32) * unscale
    for part in q_parts:
        query_sum = query_sum + part.astype(jnp.float32) * unscale

    swapped = jnp.concatenate(
        [keyval_sum[:, HEAD_DIM // 2 :], keyval_sum[:, : HEAD_DIM // 2]], axis=1
    )
    rotated = keyval_sum * cosine + swapped * sine
    own_half = jnp.where(c == 0, rotated, keyval_sum).astype(jnp.bfloat16)
    reach = n // 2
    halves = []
    for e in range(reach, 0, -1):
        halves.append(lax.ppermute(own_half, "seq", [(i, i + e) for i in range(n - e)]))
    half = jnp.concatenate(halves + [own_half], axis=0)
    other = pull(half, "sub", 1, c_size)
    docs = doc_lengths.shape[0]
    return attend(reach, docs, scalars, query_sum, cosine, sine, half, other)


def solution(mesh):
    in_specs = (
        P(("groups", "seq"), None),
        P(),
        P("seq", ("mp", "sub")),
        P("seq", ("mp", "sub")),
        P("groups"),
    )
    out_specs = P(("groups", "seq"), ("mp", "sub"))
    sizes = dict(mesh.shape)

    def body(*arrays):
        return shards(sizes, *arrays)

    return jax.shard_map(body, mesh=mesh, in_specs=in_specs, out_specs=out_specs, check_vma=False)
```

```python
import functools
import math

import jax
import jax.numpy as jnp
from jax import lax
from jax.experimental import pallas as pl
from jax.experimental.pallas import tpu as pltpu
from jax.sharding import PartitionSpec as P

HEAD_DIM = 128


NEG_LARGE = -1e30
ROPE_BASE = 500000.0
W_BOUND = 14.0
GAIN_BOUND = 1.75
WIRE_MAX = 60000.0
KERNEL_VMEM = 16 << 20


def inverse_norm(states):
    as_float = states.astype(jnp.float32)
    return lax.rsqrt(jnp.mean(as_float * as_float, axis=-1) + 1e-05)


def token_starts(positions, doc_lengths):
    doc_ends = jnp.cumsum(doc_lengths)
    begins = doc_ends - doc_lengths
    inside = begins[None, :] <= positions[:, None]
    return jnp.max(jnp.where(inside, begins[None, :], 0), axis=1)


def rope_tables(inner):
    half_dim = HEAD_DIM // 2
    frequency = jnp.exp(
        jnp.arange(half_dim, dtype=jnp.float32) * (-2.0 * math.log(ROPE_BASE) / HEAD_DIM)
    )
    angle = inner.astype(jnp.float32)[:, None] * frequency[None, :]
    cosine, sine = jnp.cos(angle), jnp.sin(angle)
    return (
        jnp.concatenate([cosine, cosine], axis=1),
        jnp.concatenate([-sine, sine], axis=1),
    )


def attend_kernel(
    reach, chunk, docs, scalars, query_ref, cos_ref, sin_ref, half_ref, other_ref, out_ref
):
    rows, count = query_ref.shape[0], half_ref.shape[0]
    heads = query_ref.shape[1] // HEAD_DIM
    first, is_key = scalars[0] * rows, scalars[1] == 0
    exponent_scale = math.log2(math.e) / math.sqrt(HEAD_DIM)
    column = first + lax.broadcasted_iota(jnp.int32, (rows, 1), 0)
    start = jnp.zeros((rows, 1), jnp.int32)
    begin = 0
    for k in range(docs):
        start = jnp.where(column >= begin, begin, start)
        begin = begin + scalars[2 + k]
    queries = []
    for h in range(heads):
        u = query_ref[:, h * HEAD_DIM : (h + 1) * HEAD_DIM]
        turned = pltpu.roll(u, HEAD_DIM // 2, 1)
        queries.append((u * cos_ref[...] + turned * sin_ref[...]).astype(jnp.bfloat16))
    for a in range(0, rows, chunk):
        low = (a + 1) // 128 * 128
        high = min(count, -(-(reach * rows + a + chunk) // 128) * 128)
        shape = (chunk, high - low)
        position = first + a + lax.broadcasted_iota(jnp.int32, shape, 0)
        key_position = first - reach * rows + low + lax.broadcasted_iota(jnp.int32, shape, 1)
        allowed = (key_position >= start[a : a + chunk]) & (key_position <= position)
        allowed = jnp.concatenate([allowed] * heads, axis=0)
        keys = jnp.where(is_key, half_ref[low:high, :], other_ref[low:high, :])
        values = jnp.where(is_key, other_ref[low:high, :], half_ref[low:high, :])
        query = jnp.concatenate([q[a : a + chunk] for q in queries], axis=0)
        scores = lax.dot_general(
            query, keys, (((1,), (1,)), ((), ())), preferred_element_type=jnp.float32
        )
        scores = jnp.where(allowed, scores, NEG_LARGE)
        top = jnp.max(scores, axis=-1, keepdims=True)
        weights = jnp.where(allowed, jnp.exp2((scores - top) * exponent_scale), 0.0)
        total = jnp.sum(weights, axis=-1, keepdims=True)
        summed = jnp.dot(weights.astype(jnp.bfloat16), values, preferred_element_type=jnp.float32)
        result = (summed / total).astype(jnp.bfloat16)
        for h in range(heads):
            columns = slice(h * HEAD_DIM, (h + 1) * HEAD_DIM)
            out_ref[a : a + chunk, columns] = result[h * chunk : (h + 1) * chunk]


def attend(reach, docs, scalars, query_sum, cosine, sine, half, other):
    rows, columns = query_sum.shape
    count = half.shape[0]
    chunk = rows
    while chunk > 16 and chunk * columns // HEAD_DIM * count > (1 << 19):
        chunk //= 2
    return pl.pallas_call(
        functools.partial(attend_kernel, reach, chunk, docs),
        out_shape=jax.ShapeDtypeStruct(query_sum.shape, jnp.bfloat16),
        in_specs=[pl.BlockSpec(memory_space=pltpu.SMEM)]
        + [pl.BlockSpec(memory_space=pltpu.VMEM)] * 5,
        out_specs=pl.BlockSpec(memory_space=pltpu.VMEM),
        cost_estimate=pl.CostEstimate(
            flops=4 * rows * count * columns,
            bytes_accessed=8 * rows * columns + 4 * count * HEAD_DIM,
            transcendentals=rows * count * columns // HEAD_DIM,
        ),
        compiler_params=pltpu.CompilerParams(vmem_limit_bytes=KERNEL_VMEM),
        name="attend",
    )(scalars, query_sum, cosine, sine, half, other)


def pull(array, axis, shift, size):
    pairs = [((i + shift) % size, i) for i in range(size)]
    return lax.ppermute(array, axis, pairs)


def dot(a, b):
    return jnp.dot(a, b, preferred_element_type=jnp.float32)


def project_kernel(scale, count, places, factor_ref, gain_ref, wq_ref, wkv_ref, *refs):
    pieces, (q_ref, kv_ref, block) = refs[:count], refs[count:]
    for i, piece in enumerate(pieces):
        for j in range(0, piece.shape[1], 128):
            chosen = pl.ds(pl.multiple_of(places[i] + j, 128), 128)
            part = piece[:, j : j + 128].astype(jnp.float32)
            normed = part * factor_ref[...] * gain_ref[:, chosen]
            block[:, chosen] = normed.astype(jnp.bfloat16)
    kv_ref[...] = dot(block[...], wkv_ref[...]) * scale
    q_ref[...] = dot(block[...], wq_ref[...]) * scale


def project(pieces, places, factor, gain, w_query, w_keyval, scale):
    rows, depth = pieces[0].shape[0], w_query.shape[0]
    widths = [piece.shape[1] for piece in pieces]
    columns = w_query.shape[1], w_keyval.shape[1]
    if any(w % 128 for w in widths):
        block = jnp.zeros((rows, depth), jnp.bfloat16)
        for piece, place in zip(pieces, places):
            block = lax.dynamic_update_slice_in_dim(block, piece, place, 1)
        block = (block.astype(jnp.float32) * factor[:, None] * gain[None, :]).astype(jnp.bfloat16)
        return dot(block, w_query) * scale, dot(block, w_keyval) * scale
    in_vmem = pl.BlockSpec(memory_space=pltpu.VMEM)
    return pl.pallas_call(
        functools.partial(project_kernel, scale, len(pieces)),
        out_shape=[jax.ShapeDtypeStruct((rows, w), jnp.float32) for w in columns],
        in_specs=[pl.BlockSpec(memory_space=pltpu.SMEM)] + [in_vmem] * (4 + len(pieces)),
        out_specs=[in_vmem, in_vmem],
        scratch_shapes=[pltpu.VMEM((rows, depth), jnp.bfloat16)],
        cost_estimate=pl.CostEstimate(
            flops=2 * rows * depth * sum(columns),
            bytes_accessed=2 * depth * sum(columns) + 2 * rows * depth,
            transcendentals=0,
        ),
        compiler_params=pltpu.CompilerParams(vmem_limit_bytes=KERNEL_VMEM),
        name="project",
    )(
        jnp.stack(places).astype(jnp.int32),
        jnp.broadcast_to(factor[:, None], (rows, 128)),
        gain[None, :],
        w_query,
        w_keyval,
        *pieces,
    )


def offsets_of(n):
    return sorted(range(1, n), key=lambda d: (min(d, n - d), d))


def shards(sizes, hidden_states, norm_gain, w_query, w_keyval, doc_lengths):
    n, m_size, c_size = sizes["seq"], sizes["mp"], sizes["sub"]
    quarters = m_size * c_size
    row_count, width = hidden_states.shape
    depth = w_query.shape[0]
    piece = depth // quarters
    s, m, c = lax.axis_index("seq"), lax.axis_index("mp"), lax.axis_index("sub")
    offsets = offsets_of(n)

    bound = GAIN_BOUND * math.sqrt(width) * W_BOUND * math.sqrt(depth)
    wire_scale = 2.0 ** min(0, math.floor(math.log2(WIRE_MAX / bound)))
    unscale = 1.0 / wire_scale

    quarter = m * c_size + c
    arrived = {}
    for d in offsets:
        column = lax.rem(s + d, n) * depth + quarter * piece
        mine = lax.dynamic_slice_in_dim(hidden_states, column, piece, 1)
        arrived[d] = pull(mine, "seq", -d, n)
    factor = inverse_norm(hidden_states)
    factors = {d: pull(factor, "seq", -d, n) for d in offsets}
    gain = lax.dynamic_slice_in_dim(norm_gain, s * depth, depth, 0)

    positions = s * row_count + jnp.arange(row_count, dtype=jnp.int32)
    starts = token_starts(positions, doc_lengths)
    cosine, sine = rope_tables(positions - starts)
    scalars = jnp.concatenate([jnp.stack([s, c]).astype(jnp.int32), doc_lengths])

    own = lax.dynamic_slice_in_dim(hidden_states, s * depth, depth, 1)
    query_sum, keyval_sum = project(
        [own], [jnp.zeros((), jnp.int32)], factor, gain, w_query, w_keyval, 1.0
    )
    places = [
        (lax.rem(m + i, m_size) * c_size + lax.rem(c + j, c_size)) * piece
        for i in range(m_size)
        for j in range(c_size)
    ]
    q_parts, kv_parts = [], []
    for d in offsets:
        pieces = []
        for i in range(m_size):
            near = pull(arrived[d], "mp", i, m_size) if i else arrived[d]
            pieces += [near]
            pieces += [pull(near, "sub", j, c_size) for j in range(1, c_size)]
        q_part, kv_part = project(pieces, places, factors[d], gain, w_query, w_keyval, wire_scale)
        kv_parts.append(pull(kv_part.astype(jnp.float16), "seq", d, n))
        q_parts.append(pull(q_part.astype(jnp.float16), "seq", d, n))
    for part in kv_parts:
        keyval_sum = keyval_sum + part.astype(jnp.float32) * unscale
    for part in q_parts:
        query_sum = query_sum + part.astype(jnp.float32) * unscale

    swapped = jnp.concatenate(
        [keyval_sum[:, HEAD_DIM // 2 :], keyval_sum[:, : HEAD_DIM // 2]], axis=1
    )
    rotated = keyval_sum * cosine + swapped * sine
    own_half = jnp.where(c == 0, rotated, keyval_sum).astype(jnp.bfloat16)
    reach = n // 2
    halves = []
    for e in range(reach, 0, -1):
        halves.append(lax.ppermute(own_half, "seq", [(i, i + e) for i in range(n - e)]))
    half = jnp.concatenate(halves + [own_half], axis=0)
    other = pull(half, "sub", 1, c_size)
    docs = doc_lengths.shape[0]
    return attend(reach, docs, scalars, query_sum, cosine, sine, half, other)


def solution(mesh):
    in_specs = (
        P(("groups", "seq"), None),
        P(),
        P("seq", ("mp", "sub")),
        P("seq", ("mp", "sub")),
        P("groups"),
    )
    out_specs = P(("groups", "seq"), ("mp", "sub"))
    sizes = dict(mesh.shape)

    def body(*arrays):
        return shards(sizes, *arrays)

    return jax.shard_map(body, mesh=mesh, in_specs=in_specs, out_specs=out_specs, check_vma=False)
```

```python
import functools
import math

import jax
import jax.numpy as jnp
from jax import lax
from jax.experimental import pallas as pl
from jax.experimental.pallas import tpu as pltpu
from jax.sharding import PartitionSpec as P

HEAD_DIM = 128


NEG_LARGE = -1e30
ROPE_BASE = 500000.0
W_BOUND = 14.0
GAIN_BOUND = 1.75
WIRE_MAX = 60000.0
KERNEL_VMEM = 16 << 20


def inverse_norm(states):
    as_float = states.astype(jnp.float32)
    return lax.rsqrt(jnp.mean(as_float * as_float, axis=-1) + 1e-05)


def token_starts(positions, doc_lengths):
    doc_ends = jnp.cumsum(doc_lengths)
    begins = doc_ends - doc_lengths
    inside = begins[None, :] <= positions[:, None]
    return jnp.max(jnp.where(inside, begins[None, :], 0), axis=1)


def rope_tables(inner):
    half_dim = HEAD_DIM // 2
    frequency = jnp.exp(
        jnp.arange(half_dim, dtype=jnp.float32) * (-2.0 * math.log(ROPE_BASE) / HEAD_DIM)
    )
    angle = inner.astype(jnp.float32)[:, None] * frequency[None, :]
    cosine, sine = jnp.cos(angle), jnp.sin(angle)
    return (
        jnp.concatenate([cosine, cosine], axis=1),
        jnp.concatenate([-sine, sine], axis=1),
    )


def attend_kernel(
    reach, chunk, docs, scalars, query_ref, cos_ref, sin_ref, half_ref, other_ref, out_ref
):
    rows, count = query_ref.shape[0], half_ref.shape[0]
    heads = query_ref.shape[1] // HEAD_DIM
    first, is_key = scalars[0] * rows, scalars[1] == 0
    exponent_scale = math.log2(math.e) / math.sqrt(HEAD_DIM)
    column = first + lax.broadcasted_iota(jnp.int32, (rows, 1), 0)
    start = jnp.zeros((rows, 1), jnp.int32)
    begin = 0
    for k in range(docs):
        start = jnp.where(column >= begin, begin, start)
        begin = begin + scalars[2 + k]
    queries = []
    for h in range(heads):
        u = query_ref[:, h * HEAD_DIM : (h + 1) * HEAD_DIM]
        turned = pltpu.roll(u, HEAD_DIM // 2, 1)
        queries.append((u * cos_ref[...] + turned * sin_ref[...]).astype(jnp.bfloat16))
    for a in range(0, rows, chunk):
        low = (a + 1) // 128 * 128
        high = min(count, -(-(reach * rows + a + chunk) // 128) * 128)
        shape = (chunk, high - low)
        position = first + a + lax.broadcasted_iota(jnp.int32, shape, 0)
        key_position = first - reach * rows + low + lax.broadcasted_iota(jnp.int32, shape, 1)
        allowed = (key_position >= start[a : a + chunk]) & (key_position <= position)
        allowed = jnp.concatenate([allowed] * heads, axis=0)
        keys = jnp.where(is_key, half_ref[low:high, :], other_ref[low:high, :])
        values = jnp.where(is_key, other_ref[low:high, :], half_ref[low:high, :])
        query = jnp.concatenate([q[a : a + chunk] for q in queries], axis=0)
        scores = lax.dot_general(
            query, keys, (((1,), (1,)), ((), ())), preferred_element_type=jnp.float32
        )
        scores = jnp.where(allowed, scores, NEG_LARGE)
        top = jnp.max(scores, axis=-1, keepdims=True)
        weights = jnp.where(allowed, jnp.exp2((scores - top) * exponent_scale), 0.0)
        total = jnp.sum(weights, axis=-1, keepdims=True)
        summed = jnp.dot(weights.astype(jnp.bfloat16), values, preferred_element_type=jnp.float32)
        result = (summed / total).astype(jnp.bfloat16)
        for h in range(heads):
            columns = slice(h * HEAD_DIM, (h + 1) * HEAD_DIM)
            out_ref[a : a + chunk, columns] = result[h * chunk : (h + 1) * chunk]


def attend(reach, docs, scalars, query_sum, cosine, sine, half, other):
    rows, columns = query_sum.shape
    count = half.shape[0]
    chunk = rows
    while chunk > 16 and chunk * columns // HEAD_DIM * count > (1 << 19):
        chunk //= 2
    return pl.pallas_call(
        functools.partial(attend_kernel, reach, chunk, docs),
        out_shape=jax.ShapeDtypeStruct(query_sum.shape, jnp.bfloat16),
        in_specs=[pl.BlockSpec(memory_space=pltpu.SMEM)]
        + [pl.BlockSpec(memory_space=pltpu.VMEM)] * 5,
        out_specs=pl.BlockSpec(memory_space=pltpu.VMEM),
        cost_estimate=pl.CostEstimate(
            flops=4 * rows * count * columns,
            bytes_accessed=8 * rows * columns + 4 * count * HEAD_DIM,
            transcendentals=rows * count * columns // HEAD_DIM,
        ),
        compiler_params=pltpu.CompilerParams(vmem_limit_bytes=KERNEL_VMEM),
        name="attend",
    )(scalars, query_sum, cosine, sine, half, other)


def pull(array, axis, shift, size):
    pairs = [((i + shift) % size, i) for i in range(size)]
    return lax.ppermute(array, axis, pairs)


def dot(a, b):
    return jnp.dot(a, b, preferred_element_type=jnp.float32)


def assemble_kernel(count, places, factor_ref, gain_ref, *refs):
    pieces, block_ref = refs[:count], refs[count]
    rows = block_ref.shape[0]
    square = (rows, rows)
    same = lax.broadcasted_iota(jnp.int32, square, 0) == lax.broadcasted_iota(jnp.int32, square, 1)
    factor = jnp.sum(jnp.where(same, factor_ref[...], 0.0), axis=1, keepdims=True)
    factor = jnp.broadcast_to(factor, (rows, 128))
    for i, piece in enumerate(pieces):
        for j in range(0, piece.shape[1], 128):
            chosen = pl.ds(pl.multiple_of(places[i] + j, 128), 128)
            part = piece[:, j : j + 128].astype(jnp.float32)
            block_ref[:, chosen] = (part * factor * gain_ref[:, chosen]).astype(jnp.bfloat16)


def assemble(pieces, places, factor, gain):
    rows, depth = pieces[0].shape[0], gain.shape[0]
    widths = [piece.shape[1] for piece in pieces]
    if any(w % 128 for w in widths):
        block = jnp.zeros((rows, depth), jnp.bfloat16)
        for piece, place in zip(pieces, places):
            block = lax.dynamic_update_slice_in_dim(block, piece, place, 1)
        return (block.astype(jnp.float32) * factor[:, None] * gain[None, :]).astype(jnp.bfloat16)
    in_vmem = pl.BlockSpec(memory_space=pltpu.VMEM)
    return pl.pallas_call(
        functools.partial(assemble_kernel, len(pieces)),
        out_shape=jax.ShapeDtypeStruct((rows, depth), jnp.bfloat16),
        in_specs=[pl.BlockSpec(memory_space=pltpu.SMEM)] + [in_vmem] * (2 + len(pieces)),
        out_specs=in_vmem,
        cost_estimate=pl.CostEstimate(
            flops=4 * rows * depth, bytes_accessed=4 * rows * depth, transcendentals=0
        ),
        compiler_params=pltpu.CompilerParams(vmem_limit_bytes=KERNEL_VMEM),
        name="assemble",
    )(jnp.stack(places).astype(jnp.int32), factor[None, :], gain[None, :], *pieces)


def groups_of(n):
    return [sorted({d, n - d}) for d in range(n // 2, 0, -1)]


def shards(sizes, hidden_states, norm_gain, w_query, w_keyval, doc_lengths):
    n, m_size, c_size = sizes["seq"], sizes["mp"], sizes["sub"]
    quarters = m_size * c_size
    row_count, width = hidden_states.shape
    depth = w_query.shape[0]
    piece = depth // quarters
    s, m, c = lax.axis_index("seq"), lax.axis_index("mp"), lax.axis_index("sub")
    offsets = [d for group in groups_of(n) for d in group]

    bound = GAIN_BOUND * math.sqrt(width) * W_BOUND * math.sqrt(depth)
    wire_scale = 2.0 ** min(0, math.floor(math.log2(WIRE_MAX / bound)))
    unscale = 1.0 / wire_scale

    quarter = m * c_size + c
    arrived = {}
    for d in offsets:
        column = lax.rem(s + d, n) * depth + quarter * piece
        mine = lax.dynamic_slice_in_dim(hidden_states, column, piece, 1)
        arrived[d] = pull(mine, "seq", -d, n)
    factor = inverse_norm(hidden_states)
    factors = {d: pull(factor, "seq", -d, n) for d in offsets}
    gain = lax.dynamic_slice_in_dim(norm_gain, s * depth, depth, 0)

    positions = s * row_count + jnp.arange(row_count, dtype=jnp.int32)
    starts = token_starts(positions, doc_lengths)
    cosine, sine = rope_tables(positions - starts)
    scalars = jnp.concatenate([jnp.stack([s, c]).astype(jnp.int32), doc_lengths])

    own = lax.dynamic_slice_in_dim(hidden_states, s * depth, depth, 1)
    own = assemble([own], [jnp.zeros((), jnp.int32)], factor, gain)
    keyval_sum, query_sum = dot(own, w_keyval), dot(own, w_query)
    places = [
        (lax.rem(m + i, m_size) * c_size + lax.rem(c + j, c_size)) * piece
        for i in range(m_size)
        for j in range(c_size)
    ]
    q_parts, kv_parts = [], []
    for d in offsets:
        pieces = []
        for i in range(m_size):
            near = pull(arrived[d], "mp", i, m_size) if i else arrived[d]
            pieces += [near]
            pieces += [pull(near, "sub", j, c_size) for j in range(1, c_size)]
        block = assemble(pieces, places, factors[d], gain)
        kv_part = (dot(block, w_keyval) * wire_scale).astype(jnp.float16)
        q_part = (dot(block, w_query) * wire_scale).astype(jnp.float16)
        kv_parts.append(pull(kv_part, "seq", d, n))
        q_parts.append(pull(q_part, "seq", d, n))
    for part in kv_parts:
        keyval_sum = keyval_sum + part.astype(jnp.float32) * unscale
    for part in q_parts:
        query_sum = query_sum + part.astype(jnp.float32) * unscale

    swapped = jnp.concatenate(
        [keyval_sum[:, HEAD_DIM // 2 :], keyval_sum[:, : HEAD_DIM // 2]], axis=1
    )
    rotated = keyval_sum * cosine + swapped * sine
    own_half = jnp.where(c == 0, rotated, keyval_sum).astype(jnp.bfloat16)
    reach = n // 2
    halves = []
    for e in range(reach, 0, -1):
        halves.append(lax.ppermute(own_half, "seq", [(i, i + e) for i in range(n - e)]))
    half = jnp.concatenate(halves + [own_half], axis=0)
    other = pull(half, "sub", 1, c_size)
    docs = doc_lengths.shape[0]
    return attend(reach, docs, scalars, query_sum, cosine, sine, half, other)


def solution(mesh):
    in_specs = (
        P(("groups", "seq"), None),
        P(),
        P("seq", ("mp", "sub")),
        P("seq", ("mp", "sub")),
        P("groups"),
    )
    out_specs = P(("groups", "seq"), ("mp", "sub"))
    sizes = dict(mesh.shape)

    def body(*arrays):
        return shards(sizes, *arrays)

    return jax.shard_map(body, mesh=mesh, in_specs=in_specs, out_specs=out_specs, check_vma=False)
```
